32 devices in a mesh: blk: 32 (over z, y, x, core).
Axes of the slice: x: 2, y: 2, z: 4, core: 2. Of those that a mesh axis runs over, the one named last changes fastest.
Arguments:
- samples: bfloat16 [8192, 2048], P('blk'), may hold values from -6 to 6
- hubs: int32 [64], replicated, may hold values from 0 to 8191, as said below
- start: int32 [1], replicated, may hold values from 1 to 13
Outputs:
- self_stat: float32 [8192, 256], P('blk')
- ahead_stat: float32 [3, 8192, 256], P(None, 'blk')
- behind_stat: float32 [3, 8192, 256], P(None, 'blk')
The draws below stay inside these ranges and needn't reach their ends.
Inputs may be any that keep to these rules, and one draw needn't show every extreme that they name: `hubs`: the 64 indices are distinct.
All inputs are finite; a program needn't handle non-finite values.
Results may differ from the reference program's by a relative error of at most 0.0049.
Values may be sent and summed in bfloat16 or wider, within the bound.
No kernel may reach another device: no remote copies, remote signals or barrier semaphores. Data moves between devices by JAX's collectives and lax.ppermute only.
A program may use at most 64 MiB of HBM per device.

```python
import math
import jax
import jax.numpy as jnp
from jax import lax

BLK = 256
SAMPLES = 2048
HUBS = 64
WINDOW = 3
TRANSCRIPTS = 8192
N_BLK = 32


def draw_hubs(key, part):
    order = jax.random.permutation(jax.random.fold_in(key, 11), TRANSCRIPTS)
    return order[:HUBS].astype(jnp.int32)


def block_levels(key, extent, pieces, smallest, top_value):
    factor_of, own = 1.0, jax.random.fold_in(key, 6)
    for position, parts in pieces:
        draws = jnp.exp(jax.random.uniform(jax.random.fold_in(own, position), (parts,), jnp.float32, smallest / len(pieces), top_value / len(pieces)))
        factor_of = factor_of * jnp.repeat(draws, extent[position] // parts).reshape([-1 if axis == position else 1 for axis in range(len(extent))])
    return factor_of


def noise(rng, shape, deviation, bound, pieces=(), kind=jnp.bfloat16):
    values = deviation * jax.random.normal(rng, shape, jnp.float32)
    if pieces:
        values = values * block_levels(rng, shape, pieces, -0.22, 0.18)
    return jnp.clip(values, -bound, bound).astype(kind)


def setup_inputs(seed: int = 0) -> dict:
    splits = jax.random.split(jax.random.key(seed), 4)
    return {
        "samples": noise(splits[0], (TRANSCRIPTS, SAMPLES), 1.0, 6.0, ((0, 32),)),
        "hubs": draw_hubs(jax.random.fold_in(splits[3], 71), 0),
        "start": jax.random.randint(splits[2], (1,), 1, N_BLK // 2 - 2).astype(jnp.int32),
    }


def fisher(values):
    return 0.5 * (jnp.log1p(values) - jnp.log1p(-values))

def reference(samples, hubs, start):
    hub_rows = samples[hubs].astype(jnp.float32)
    gram = jnp.dot(hub_rows, hub_rows.T, precision=lax.Precision.HIGHEST)
    proj = jnp.dot(samples.astype(jnp.float32), hub_rows.astype(jnp.bfloat16).T.astype(jnp.float32), preferred_element_type=jnp.float32)
    coef = jnp.linalg.solve(gram, proj.T).T
    resid = (samples.astype(jnp.float32) - jnp.dot(coef, hub_rows, precision=lax.Precision.HIGHEST)).astype(jnp.bfloat16)
    wide = resid.astype(jnp.float32)
    scale = 1.0 / jnp.sqrt(jnp.maximum(lax.optimization_barrier(jnp.sum(wide * wide, axis=1)), 1.0))
    blocks = wide.reshape(N_BLK, BLK, SAMPLES)
    scales = scale.reshape(N_BLK, BLK)
    factor = math.sqrt(SAMPLES - HUBS - 3)

    def corr_for(offset):
        other = jnp.roll(blocks, -offset, axis=0)
        other_scale = jnp.roll(scales, -offset, axis=0)
        dots = jnp.einsum('bis,bks->bik', blocks, other)
        return (dots * scales[:, :, None] * other_scale[:, None, :]).astype(jnp.bfloat16)

    def to_stat(rounded):
        return factor * fisher(lax.optimization_barrier(rounded).astype(jnp.float32))
    own = corr_for(jnp.int32(0))
    diag = jnp.eye(BLK, dtype=jnp.bool_)[None, :, :]
    own_stat = jnp.where(diag, 0.0, to_stat(own))
    ahead = []
    behind = []
    for j in range(WINDOW):
        offset = start[0] + j
        tiles = corr_for(offset)
        ahead.append(to_stat(tiles).reshape(TRANSCRIPTS, BLK))
        turned = jnp.transpose(jnp.roll(tiles, offset, axis=0), (0, 2, 1))
        behind.append(to_stat(turned).reshape(TRANSCRIPTS, BLK))
    return (own_stat.reshape(TRANSCRIPTS, BLK), jnp.stack(ahead), jnp.stack(behind))
```

```python
import functools
import math

import jax
import jax.numpy as jnp
from jax import lax
from jax.experimental import pallas as pl
from jax.experimental.pallas import tpu as pltpu
from jax.sharding import PartitionSpec as P

WINDOW = 3
RADIX = 16


def route(block, pairs):
    return lax.ppermute(block, "blk", pairs)


def shifted(block, distance):
    count = lax.axis_size("blk")
    if distance % count == 0:
        return block
    return route(block, [((i - distance) % count, i) for i in range(count)])


def crossed(block, mask):
    return route(block, [(i ^ mask, i) for i in range(lax.axis_size("blk"))])


def plan(offset):
    rest = offset % 4
    far = offset - rest if rest < 2 else offset - rest + 4
    return far, offset - far


def to_stat(rounded, factor):
    values = lax.optimization_barrier(rounded).astype(jnp.float32)
    return factor * (0.5 * (jnp.log1p(values) - jnp.log1p(-values)))


def gather_hubs(parts):
    own = parts[0]
    for k in (1, 2, 3):
        own = own + crossed(parts[k], k)
    mask = 4
    while mask < lax.axis_size("blk"):
        own = own + crossed(own, mask)
        mask *= 2
    return jnp.concatenate([own] + [crossed(own, k) for k in (1, 2, 3)])


def inverse_gram(hub_rows):
    gram = lax.dot_general(
        hub_rows, hub_rows, (((1,), (1,)), ((), ())), preferred_element_type=jnp.float32
    )
    lower = jnp.linalg.cholesky(gram)
    inv_lower = jax.scipy.linalg.solve_triangular(
        lower, jnp.eye(gram.shape[0], dtype=jnp.float32), lower=True
    )
    return jnp.dot(inv_lower.T, inv_lower, precision=lax.Precision.HIGHEST)


def near_blocks(samples, first):
    count = lax.axis_size("blk")
    odd = lax.axis_index("blk") % 2 == 1
    if first == -1:
        return shifted(samples, -1), samples, shifted(samples, 1)
    if first == -2:
        two = shifted(samples, -2)
        one = crossed(jnp.where(odd, samples, two), 1)
        return two, one, samples
    two = shifted(samples, 2)
    one = crossed(jnp.where(odd, two, samples), 1)
    if first == 0:
        return samples, one, two
    three_even = route(samples, [((i - 3) % count, i) for i in range(0, count, 2)])
    three_odd = route(two, [(i, i + 1) for i in range(0, count, 2)])
    return one, two, jnp.where(odd, three_odd, three_even)


def exchange(offset, samples, parts):
    far_distance, first = plan(offset)
    hub_rows = gather_hubs(parts)
    far = shifted(samples, -far_distance)
    near = near_blocks(samples, first)
    return (hub_rows, inverse_gram(hub_rows), far) + near


def give_back(offset, tiles, turned):
    far_distance, first = plan(offset)
    ahead = [shifted(tiles[j], -(first + j)) for j in range(WINDOW)]
    return tuple(ahead), shifted(turned, far_distance)


def residual(x_ref, hub_rows, inverse, out_ref, step):
    proj = lax.dot_general(
        x_ref[...], hub_rows, (((1,), (1,)), ((), ())), preferred_element_type=jnp.float32
    )
    coef = jnp.dot(
        proj, inverse, precision=lax.Precision.HIGHEST, preferred_element_type=jnp.float32
    )
    high = coef.astype(jnp.bfloat16)
    rest = coef - high.astype(jnp.float32)
    mid = rest.astype(jnp.bfloat16)
    low = (rest - mid.astype(jnp.float32)).astype(jnp.bfloat16)
    total = jnp.zeros((x_ref.shape[0], 1), jnp.float32)
    for at in range(0, x_ref.shape[1], step):
        part = hub_rows[:, at:at + step]
        fit = jnp.dot(low, part, preferred_element_type=jnp.float32)
        fit = fit + jnp.dot(mid, part, preferred_element_type=jnp.float32)
        fit = fit + jnp.dot(high, part, preferred_element_type=jnp.float32)
        resid = (x_ref[:, at:at + step].astype(jnp.float32) - fit).astype(jnp.bfloat16)
        out_ref[:, at:at + step] = resid
        wide = resid.astype(jnp.float32)
        total = total + jnp.sum(wide * wide, axis=1, keepdims=True)
    return 1.0 / jnp.sqrt(jnp.maximum(total, 1.0))


def tiles_kernel(
    own_ref, far_ref, near0_ref, near1_ref, near2_ref, hub_ref, inv_ref,
    self_ref, tile_ref, turned_ref, one_ref, two_ref,
):
    hub_rows = hub_ref[...]
    inverse = inv_ref[...]
    step = 512
    rows = own_ref.shape[0]

    def row_of(scale):
        return jnp.transpose(jnp.broadcast_to(scale, (rows, 128)))[0:1, :]

    def corr(left, left_scale, right, right_row):
        dots = lax.dot_general(
            left[...], right[...], (((1,), (1,)), ((), ())), preferred_element_type=jnp.float32
        )
        return dots * left_scale * right_row

    scale = residual(own_ref, hub_rows, inverse, one_ref, step)
    self_ref[...] = corr(one_ref, scale, one_ref, row_of(scale)).astype(jnp.bfloat16)
    far_scale = residual(far_ref, hub_rows, inverse, two_ref, step)
    far_row = row_of(far_scale)
    for j, near_ref in enumerate((near0_ref, near1_ref, near2_ref)):
        scale = residual(near_ref, hub_rows, inverse, one_ref, step)
        tile = corr(one_ref, scale, two_ref, far_row)
        tile_ref[j] = tile.astype(jnp.bfloat16)
        turned_ref[j] = jnp.transpose(tile).astype(jnp.bfloat16)


def make_tiles(own, far, near, hub_rows, inverse):
    rows, width = own.shape
    vmem = pl.BlockSpec(memory_space=pltpu.VMEM)
    return pl.pallas_call(
        tiles_kernel,
        out_shape=(
            jax.ShapeDtypeStruct((rows, rows), jnp.bfloat16),
            jax.ShapeDtypeStruct((WINDOW, rows, rows), jnp.bfloat16),
            jax.ShapeDtypeStruct((WINDOW, rows, rows), jnp.bfloat16),
        ),
        in_specs=[vmem] * 7,
        out_specs=(vmem, vmem, vmem),
        scratch_shapes=[
            pltpu.VMEM((rows, width), jnp.bfloat16),
            pltpu.VMEM((rows, width), jnp.bfloat16),
        ],
        name="tiles",
    )(own, far, *near, hub_rows, inverse)


def shards(samples, hubs, start):
    rows, width = samples.shape
    factor = math.sqrt(width - hubs.shape[0] - 3)
    count = lax.axis_size("blk")
    mine = lax.axis_index("blk")
    offset = start[0]

    quad = jnp.bitwise_xor(mine % 4, jnp.arange(4, dtype=jnp.int32))
    wanted = hubs.reshape(4, -1)[quad].reshape(-1) - mine * rows
    picker = (wanted[:, None] == jnp.arange(rows, dtype=jnp.int32)[None, :]).astype(jnp.bfloat16)
    held = jnp.dot(picker, samples, preferred_element_type=jnp.float32).astype(jnp.bfloat16)
    parts = tuple(jnp.split(held, 4))

    largest = count // 2 - WINDOW
    if largest < RADIX:
        lows, index, highs = range(1, largest + 1), offset - 1, 1
    else:
        lows, index, highs = range(RADIX), offset % RADIX, largest // RADIX + 1
    hops = [functools.partial(shifted, distance=-RADIX * k) for k in range(highs)]
    back_hops = [functools.partial(shifted, distance=RADIX * k) for k in range(highs)]

    hub_rows, inverse, far, *near = lax.switch(
        index, [functools.partial(exchange, low) for low in lows], samples, parts
    )
    if highs > 1:
        far = lax.switch(offset // RADIX, hops, far)

    own, tiles, turned = make_tiles(samples, far, near, hub_rows, inverse)

    ahead, behind = lax.switch(
        index, [functools.partial(give_back, low) for low in lows], tiles, turned
    )
    if highs > 1:
        behind = lax.switch(offset // RADIX, back_hops, behind)

    diag = jnp.arange(rows)[:, None] == jnp.arange(rows)[None, :]
    own_stat = jnp.where(diag, 0.0, to_stat(own, factor))
    ahead = jnp.stack([to_stat(tile, factor) for tile in ahead])
    return (own_stat, ahead, to_stat(behind, factor))


def solution(mesh):
    in_specs = (P("blk", None), P(), P())
    out_specs = (P("blk", None), P(None, "blk", None), P(None, "blk", None))
    return jax.shard_map(shards, mesh=mesh, in_specs=in_specs, out_specs=out_specs, check_vma=False)
```

```python
import functools
import math

import jax
import jax.numpy as jnp
from jax import lax
from jax.experimental import pallas as pl
from jax.experimental.pallas import tpu as pltpu
from jax.sharding import PartitionSpec as P

WINDOW = 3
RADIX = 16


def route(block, pairs):
    return lax.ppermute(block, "blk", pairs)


def shifted(block, distance):
    count = lax.axis_size("blk")
    if distance % count == 0:
        return block
    return route(block, [((i - distance) % count, i) for i in range(count)])


def crossed(block, mask):
    return route(block, [(i ^ mask, i) for i in range(lax.axis_size("blk"))])


def to_stat(rounded, factor):
    values = rounded.astype(jnp.float32)
    return factor * (0.5 * (jnp.log1p(values) - jnp.log1p(-values)))


def gather_hubs(parts):
    own = parts[0]
    for k in (1, 2, 3):
        own = own + crossed(parts[k], k)
    mask = 4
    while mask < lax.axis_size("blk"):
        own = own + crossed(own, mask)
        mask *= 2
    return jnp.concatenate([own] + [crossed(own, k) for k in (1, 2, 3)])


def inverse_gram(hub_rows):
    gram = lax.dot_general(
        hub_rows, hub_rows, (((1,), (1,)), ((), ())), preferred_element_type=jnp.float32
    )
    across = lax.broadcasted_iota(jnp.int32, gram.shape, 1)
    down = lax.broadcasted_iota(jnp.int32, gram.shape, 0)

    def sweep(k, held):
        in_row, in_col = down == k, across == k
        row = jnp.sum(jnp.where(in_row, held, 0.0), axis=0, keepdims=True)
        col = jnp.sum(jnp.where(in_col, held, 0.0), axis=1, keepdims=True)
        pivot = 1.0 / jnp.sum(jnp.where(across[0:1] == k, row, 0.0), axis=1, keepdims=True)
        scaled = row * pivot
        new = jnp.where(in_col, col * pivot, held - col * scaled)
        new = jnp.where(in_row, scaled, new)
        return jnp.where(jnp.logical_and(in_row, in_col), -pivot, new)

    return -lax.fori_loop(0, gram.shape[0], sweep, gram)


def pieces(proj, inverse):
    coef = jnp.dot(
        proj, inverse, precision=lax.Precision.HIGHEST, preferred_element_type=jnp.float32
    )
    high = coef.astype(jnp.bfloat16)
    rest = coef - high.astype(jnp.float32)
    mid = rest.astype(jnp.bfloat16)
    low = (rest - mid.astype(jnp.float32)).astype(jnp.bfloat16)
    return jnp.concatenate([high, mid, low], axis=1)


def loop(steps, body, init, rolled):
    if rolled:
        return lax.fori_loop(0, steps, body, init)
    for k in range(steps):
        init = body(k, init)
    return init


def residual(x_ref, hub_ref, inverse, out_ref, step, rolled):
    rows, width = x_ref.shape

    def at(k):
        return pl.ds(pl.multiple_of(k * step, step) if rolled else k * step, step)

    def project(k, proj):
        return proj + lax.dot_general(
            x_ref[:, at(k)], hub_ref[:, at(k)], (((1,), (1,)), ((), ())),
            preferred_element_type=jnp.float32,
        )

    if rolled:
        proj = loop(
            width // step, project, jnp.zeros((rows, hub_ref.shape[0]), jnp.float32), rolled
        )
    else:
        proj = lax.dot_general(
            x_ref[...], hub_ref[...], (((1,), (1,)), ((), ())), preferred_element_type=jnp.float32
        )
    coef = pieces(proj, inverse)

    def subtract(k, total):
        part = hub_ref[:, at(k)]
        fit = jnp.dot(
            coef, jnp.concatenate([part] * 3, axis=0), preferred_element_type=jnp.float32
        )
        resid = (x_ref[:, at(k)].astype(jnp.float32) - fit).astype(jnp.bfloat16)
        out_ref[:, at(k)] = resid
        wide = resid.astype(jnp.float32)
        square = wide * wide
        for lane in range(0, step, 128):
            total = total + square[:, lane:lane + 128]
        return total

    total = loop(width // step, subtract, jnp.zeros((rows, 128), jnp.float32), rolled)
    total = jnp.sum(total, axis=1, keepdims=True)
    return 1.0 / jnp.sqrt(jnp.maximum(total, 1.0))


def as_row(scale):
    return jnp.transpose(jnp.broadcast_to(scale, (scale.shape[0], 128)))[0:1, :]


def correlation(left_ref, left_scale, right_ref, right_row, step, rolled):
    rows, width = left_ref.shape

    def add(k, dots):
        at = pl.ds(pl.multiple_of(k * step, step) if rolled else k * step, step)
        return dots + lax.dot_general(
            left_ref[:, at], right_ref[:, at], (((1,), (1,)), ((), ())),
            preferred_element_type=jnp.float32,
        )

    if rolled:
        dots = loop(width // step, add, jnp.zeros((rows, rows), jnp.float32), rolled)
    else:
        dots = lax.dot_general(
            left_ref[...], right_ref[...], (((1,), (1,)), ((), ())),
            preferred_element_type=jnp.float32,
        )
    return dots * left_scale * right_row


def own_kernel(factor, own_ref, hub_ref, inv_ref, self_ref, resid_ref, scale_ref):
    inverse = inverse_gram(hub_ref[...])
    inv_ref[...] = inverse
    scale = residual(own_ref, hub_ref, inverse, resid_ref, 256, True)
    scale_ref[...] = scale
    tile = correlation(resid_ref, scale, resid_ref, as_row(scale), 256, True)
    stat = to_stat(tile.astype(jnp.bfloat16), factor)
    down = lax.broadcasted_iota(jnp.int32, stat.shape, 0)
    across = lax.broadcasted_iota(jnp.int32, stat.shape, 1)
    self_ref[...] = jnp.where(down == across, 0.0, stat)


def own_tile(own, hub_rows, factor):
    rows, width = own.shape
    hubs = hub_rows.shape[0]
    vmem = pl.BlockSpec(memory_space=pltpu.VMEM)
    return pl.pallas_call(
        functools.partial(own_kernel, factor),
        out_shape=(
            jax.ShapeDtypeStruct((hubs, hubs), jnp.float32),
            jax.ShapeDtypeStruct((rows, rows), jnp.float32),
            jax.ShapeDtypeStruct((rows, width), jnp.bfloat16),
            jax.ShapeDtypeStruct((rows, 1), jnp.float32),
        ),
        in_specs=[vmem] * 2,
        out_specs=(vmem,) * 4,
        cost_estimate=pl.CostEstimate(
            flops=20 * 10**9, bytes_accessed=2 * rows * width, transcendentals=0
        ),
        name="own_tile",
    )(own, hub_rows)


def tiles_kernel(
    far_ref, next_ref, own_ref, scale_ref, last_ref, hub_ref, inv_ref,
    tile_ref, turned_ref, one_ref, two_ref,
):
    inverse = inv_ref[...]
    far_row = as_row(residual(far_ref, hub_ref, inverse, two_ref, 512, False))
    for j, near_ref in enumerate((next_ref, None, last_ref)):
        if near_ref is None:
            left, scale = own_ref, scale_ref[...]
        else:
            left, scale = one_ref, residual(near_ref, hub_ref, inverse, one_ref, 512, False)
        tile = correlation(left, scale, two_ref, far_row, 512, False)
        tile_ref[j] = tile.astype(jnp.bfloat16)
        turned_ref[j] = jnp.transpose(tile).astype(jnp.bfloat16)


def make_tiles(far, *rest):
    rows, width = far.shape
    vmem = pl.BlockSpec(memory_space=pltpu.VMEM)
    return pl.pallas_call(
        tiles_kernel,
        out_shape=(jax.ShapeDtypeStruct((WINDOW, rows, rows), jnp.bfloat16),) * 2,
        in_specs=[vmem] * 7,
        out_specs=(vmem,) * 2,
        scratch_shapes=[pltpu.VMEM((rows, width), jnp.bfloat16)] * 2,
        name="tiles",
    )(far, *rest)


def stats_kernel(factor, next_ref, own_ref, last_ref, back_ref, ahead_ref, behind_ref):
    for j, tile_ref in enumerate((next_ref, own_ref, last_ref)):
        ahead_ref[j] = to_stat(tile_ref[...], factor)
        behind_ref[j] = to_stat(back_ref[j], factor)


def make_stats(ahead, back, factor):
    vmem = pl.BlockSpec(memory_space=pltpu.VMEM)
    return pl.pallas_call(
        functools.partial(stats_kernel, factor),
        out_shape=(jax.ShapeDtypeStruct(back.shape, jnp.float32),) * 2,
        in_specs=[vmem] * 4,
        out_specs=(vmem,) * 2,
        name="stats",
    )(*ahead, back)


def exchange(offset, samples, hub_rows, factor):
    far = shifted(samples, -(offset + 1))
    following = shifted(samples, -1)
    previous = shifted(samples, 1)
    return own_tile(samples, hub_rows, factor) + (far, following, previous)


def give_back(offset, tiles, turned):
    ahead = (shifted(tiles[0], 1), tiles[1], shifted(tiles[2], -1))
    return ahead, shifted(turned, offset + 1)


def shards(samples, hubs, start):
    rows, width = samples.shape
    factor = math.sqrt(width - hubs.shape[0] - 3)
    count = lax.axis_size("blk")
    mine = lax.axis_index("blk")
    offset = start[0]

    quad = jnp.bitwise_xor(mine % 4, jnp.arange(4, dtype=jnp.int32))
    wanted = hubs.reshape(4, -1)[quad].reshape(-1) - mine * rows
    picker = (wanted[:, None] == jnp.arange(rows, dtype=jnp.int32)[None, :]).astype(jnp.bfloat16)
    held = jnp.dot(picker, samples, preferred_element_type=jnp.float32).astype(jnp.bfloat16)
    parts = tuple(jnp.split(held, 4))

    largest = count // 2 - WINDOW
    if largest < RADIX:
        lows, index, highs = range(1, largest + 1), offset - 1, 1
    else:
        lows, index, highs = range(RADIX), offset % RADIX, largest // RADIX + 1
    hops = [functools.partial(shifted, distance=-RADIX * k) for k in range(highs)]
    back_hops = [functools.partial(shifted, distance=RADIX * k) for k in range(highs)]

    hub_rows = gather_hubs(parts)
    inverse, own_stat, own, scale, far, following, previous = lax.switch(
        index, [functools.partial(exchange, low, factor=factor) for low in lows],
        samples, hub_rows,
    )
    if highs > 1:
        far = lax.switch(offset // RADIX, hops, far)

    tiles, turned = make_tiles(far, following, own, scale, previous, hub_rows, inverse)

    ahead, back = lax.switch(
        index, [functools.partial(give_back, low) for low in lows], tiles, turned
    )
    if highs > 1:
        back = lax.switch(offset // RADIX, back_hops, back)
    return (own_stat,) + tuple(make_stats(ahead, back, factor))


def solution(mesh):
    in_specs = (P("blk", None), P(), P())
    out_specs = (P("blk", None), P(None, "blk", None), P(None, "blk", None))
    return jax.shard_map(shards, mesh=mesh, in_specs=in_specs, out_specs=out_specs, check_vma=False)
```
